32 devices in a mesh: dp: 8 (over z, y), comp: 4 (over x, core).
Axes of the slice: x: 2, y: 2, z: 4, core: 2. Of those that a mesh axis runs over, the one named last changes fastest.
Arguments:
- points: float32 [8192, 128], P('dp'), may hold values from -64 to 64
- block_counts: int32 [8], replicated, may hold values from 1 to 16, as said below
- block_dest: int32 [8, 16], replicated, may hold values from 0 to 7, as said below
- means: float32 [256, 128], P(('dp', 'comp')), may hold values from -3 to 3
- factors: float32 [256, 128, 128], P(('dp', 'comp')), may hold values from -0.25 to 1.4, as said below
- log_weights: float32 [256], P(('dp', 'comp')), may hold values from -4 to 4
Outputs:
- new_means: float32 [256, 128], P(('dp', 'comp'))
- new_factors: float32 [256, 128, 128], P(('dp', 'comp'))
- new_log_weights: float32 [256], P(('dp', 'comp'))
- log_density: float32 [2048], P('dp')
The draws below stay inside these ranges and needn't reach their ends.
Inputs may be any that keep to these rules, and one draw needn't show every extreme that they name: `block_counts`: blocks live on each index of dp on entry; they sum to 32, and one index holds exactly 16. `block_dest`: for j < block_counts[s], the index of dp that receives block j of index s; every index receives exactly 4 blocks, no index sends more than 2 blocks to one index, and some index sends exactly 2 to one; entries with j >= block_counts[s] are unused. `factors`: each matrix is upper triangular with diagonal entries from 0.7 to 1.4.
All inputs are finite; a program needn't handle non-finite values.
Results may differ from the reference program's by a relative error of at most 0.003.
Values sent between devices are 32-bit elements; how exact they have to be, the bound alone decides.
A program may use at most 128 MiB of HBM per device.

```python
import math
import jax
import jax.numpy as jnp
from jax import lax

D = 128
K = 256
BR = 64
RB = 4
ITERS = 2
NB = 16
N_DP = 8


def layout_tables(key):
    base_key = jax.random.fold_in(key, 7)
    key_hot, key_moves, key_perm = jax.random.split(base_key, 3)
    hottest = jax.random.randint(key_hot, (), 0, N_DP).astype(jnp.int32)
    counts = jnp.full((N_DP,), RB, jnp.int32)
    device_ids = jnp.arange(N_DP, dtype=jnp.int32)

    def lift(turn_index, current):
        others = jnp.where(device_ids == hottest, -1, current)
        donor_index = jnp.argmax(others).astype(jnp.int32)
        amount = (current[hottest] < NB).astype(jnp.int32)
        return current.at[donor_index].add(-amount).at[hottest].add(amount)
    counts = lax.fori_loop(0, NB, lift, counts)
    move_total = 8 * N_DP * RB
    move_pairs = jax.random.randint(key_moves, (move_total, 2), 0, N_DP).astype(jnp.int32)

    def wander(turn_index, current):
        donor_index = move_pairs[turn_index, 0]
        taker_index = move_pairs[turn_index, 1]
        allowed = (current[donor_index] > 1) & (current[taker_index] < NB - 1) & (donor_index != taker_index)
        allowed = allowed & (donor_index != hottest) & (taker_index != hottest)
        amount = allowed.astype(jnp.int32)
        return current.at[donor_index].add(-amount).at[taker_index].add(amount)
    counts = lax.fori_loop(0, move_total, wander, counts)
    positions = jnp.arange(NB, dtype=jnp.int32)
    prefix = jnp.cumsum(counts).astype(jnp.int32) - counts
    order_index = prefix[:, None] + positions[None, :]
    shuffle = jax.random.permutation(key_perm, N_DP).astype(jnp.int32)
    return (counts, shuffle[order_index % N_DP])


def draw_block_counts(key, part):
    return layout_tables(key)[0]


def draw_block_dest(key, part):
    return layout_tables(key)[1]


def draw_points(key, part):
    base_draw = jnp.clip(jax.random.normal(key, (N_DP * NB * BR, D), jnp.float32), -6.0, 6.0)
    return base_draw


def draw_factors(key, part):
    diag_key = jax.random.fold_in(key, 11)
    off_key = jax.random.fold_in(key, 13)
    diagonal = jax.random.uniform(diag_key, (K, D), jnp.float32, 0.7, 1.4)
    spread = jnp.clip(jax.random.normal(off_key, (K, D, D), jnp.float32), -4.0, 4.0) * (0.35 / D ** 0.5)
    return jnp.triu(spread, 1) + diagonal[:, :, None] * jnp.eye(D, dtype=jnp.float32)


def level_of(rng, shape, shards, smallest, high):
    def one(axis_at, blocks):
        steps = jax.random.uniform(jax.random.fold_in(jax.random.fold_in(rng, 6), axis_at), (blocks,), jnp.float32, smallest / len(shards), high / len(shards))
        return jnp.repeat(jnp.exp(steps), shape[axis_at] // blocks).reshape((-1,) + (1,) * (len(shape) - axis_at - 1))

    gain = one(*shards[0])
    for cut in shards[1:]:
        gain = gain * one(*cut)
    return gain


def noise(key, extent, width, reach, pieces=(), kind=jnp.bfloat16):
    drawn = width * jax.random.normal(key, extent, jnp.float32)
    if pieces:
        drawn = drawn * level_of(key, extent, pieces, -0.22, 0.18)
    return jnp.clip(drawn, -reach, reach).astype(kind)


def setup_inputs(seed: int = 0) -> dict:
    keys = jax.random.split(jax.random.key(seed), 7)
    points = draw_points(jax.random.fold_in(keys[6], 71), 0)
    block_counts = draw_block_counts(jax.random.fold_in(keys[6], 71), 0)
    block_dest = draw_block_dest(jax.random.fold_in(keys[6], 71), 0)
    means = noise(keys[3], (K, D), 0.5, 3.0, ((0, 32),), jnp.float32)
    factors = draw_factors(jax.random.fold_in(keys[6], 71), 0)
    log_weights = noise(keys[5], (K,), 1.0, 4.0, ((0, 32),), jnp.float32)
    return dict(points=points, block_counts=block_counts, block_dest=block_dest, means=means, factors=factors, log_weights=log_weights)


highest = lax.Precision.HIGHEST
ridge_term = 1.0
log_two_pi = math.log(2.0 * math.pi)

def rebalance(points, block_counts, block_dest):
    blocks = points.reshape(N_DP * NB, BR, D)
    positions = jnp.arange(NB, dtype=jnp.int32)
    live_flag = (positions[None, :] < block_counts[:, None]).reshape(-1)
    targets = block_dest.reshape(-1).astype(jnp.int32)
    devices = jnp.arange(N_DP, dtype=jnp.int32)
    target_hits = ((targets[:, None] == devices[None, :]) & live_flag[:, None]).astype(jnp.int32)
    earlier = jnp.cumsum(target_hits, axis=0).astype(jnp.int32) - target_hits
    block_rank = jnp.sum(earlier * target_hits, axis=1).astype(jnp.int32)
    places = jnp.where(live_flag, targets * RB + block_rank, N_DP * RB).astype(jnp.int32)
    placed = jnp.zeros((N_DP * RB, BR, D), jnp.float32).at[places].set(blocks, mode='drop')
    return placed.reshape(N_DP * RB * BR, D)

def component_density(points_live, centres, factor_set, weights):

    def single(inputs):
        centre, factor, weight = inputs
        projected = jnp.dot(points_live - centre[None, :], factor, precision=highest)
        logdet = jnp.sum(jnp.log(jnp.diagonal(factor)))
        return weight + logdet - 0.5 * D * log_two_pi - 0.5 * jnp.sum(projected * projected, axis=1)
    return lax.map(single, (centres, factor_set, weights))

def moments(points_live, centres, responsibility):

    def single(inputs):
        centre, weight_row = inputs
        shifted = points_live - centre[None, :]
        weight_sum = jnp.sum(weight_row)
        first_moment = jnp.dot(weight_row, shifted, precision=highest)
        second_moment = lax.dot_general(shifted * weight_row[:, None], shifted, (((0,), (0,)), ((), ())), precision=highest)
        return (weight_sum, first_moment, second_moment)
    return lax.map(single, (centres, responsibility))

def refresh(centres, weight_sum, first_moment, second_moment, total_points):
    identity = jnp.eye(centres.shape[1], dtype=jnp.float32)
    counted = weight_sum + 1.0
    covariance = (second_moment - first_moment[:, :, None] * first_moment[:, None, :] / counted[:, None, None] + ridge_term * identity) / counted[:, None, None]
    cholesky_lower = jnp.linalg.cholesky(covariance)
    inverse_lower = jax.scipy.linalg.solve_triangular(cholesky_lower, jnp.broadcast_to(identity, covariance.shape), lower=True)
    return (centres + first_moment / counted[:, None], jnp.swapaxes(inverse_lower, 1, 2), jnp.log(counted / total_points))

def reference(points, block_counts, block_dest, means, factors, log_weights):
    points_live = rebalance(points, block_counts, block_dest)
    total_points = float(N_DP * RB * BR + K)
    centres, factor_set, weights = (means, factors, log_weights)
    log_total = jnp.zeros((N_DP * RB * BR,), jnp.float32)
    for iteration in range(ITERS):
        log_table = component_density(points_live, centres, factor_set, weights)
        row_peak = jnp.max(log_table, axis=0)
        log_total = row_peak + jnp.log(jnp.sum(jnp.exp(log_table - row_peak[None, :]), axis=0))
        responsibility = jnp.exp(log_table - log_total[None, :])
        weight_sum, first_moment, second_moment = moments(points_live, centres, responsibility)
        centres, factor_set, weights = refresh(centres, weight_sum, first_moment, second_moment, total_points)
    return (centres, factor_set, weights, log_total / D)
```

```python
import math

import jax
import jax.numpy as jnp
from jax import lax
from jax.experimental import pallas as pl
from jax.experimental.pallas import tpu as pltpu
from jax.sharding import PartitionSpec as P

ITERS = 2

density_precision = lax.Precision.HIGHEST
moment_precision = lax.Precision.HIGHEST
log_two_pi = math.log(2.0 * math.pi)
PARAMS = pltpu.CompilerParams(vmem_limit_bytes=56 * 1024 * 1024)
VMEM = pl.BlockSpec(memory_space=pltpu.VMEM)
SMEM = pl.BlockSpec(memory_space=pltpu.SMEM)
ANY = pl.BlockSpec(memory_space=pl.ANY)
PANEL = 8


def talking(number):
    return pltpu.CompilerParams(
        vmem_limit_bytes=56 * 1024 * 1024, collective_id=number, has_side_effects=True
    )


MESH = pl.DeviceIdType.MESH


def here():
    comps = lax.axis_size("comp")
    return lax.axis_index("dp") * comps + lax.axis_index("comp")


def device(flat):
    comps = lax.axis_size("comp")
    return {"dp": flat // comps, "comp": flat % comps}


def device_count():
    return lax.axis_size("dp") * lax.axis_size("comp")


def greet():
    devices = device_count()
    me = here()
    barrier = pltpu.get_barrier_semaphore()

    def one(d, carry):
        pl.semaphore_signal(
            barrier, inc=1, device_id=device((me + d) % devices), device_id_type=MESH
        )
        return carry

    lax.fori_loop(1, devices, one, 0)


def greeted():
    pl.semaphore_wait(pltpu.get_barrier_semaphore(), device_count() - 1)


def remote(src, dst, send_sem, recv_sem, where):
    return pltpu.make_async_remote_copy(
        src_ref=src, dst_ref=dst, send_sem=send_sem, recv_sem=recv_sem,
        device_id=where, device_id_type=MESH,
    )


def gather_stage(
    counts_ref, dest_ref, points_ref, x_ref,
    part_ref, out_ref, in_ref, mine_ref,
    load_sem, sent, came, spread_sent, spread_came, pair_sent, pair_came, own_sem,
):
    groups = lax.axis_size("dp")
    comps = lax.axis_size("comp")
    nblocks, share, width = part_ref.shape
    slots = out_ref.shape[1]
    places = mine_ref.shape[0]
    e = lax.axis_index("dp")
    c = lax.axis_index("comp")

    load = pltpu.make_async_copy(
        points_ref.at[:, pl.ds(pl.multiple_of(c * share, share), share), :], part_ref, load_sem
    )
    load.start()
    load.wait()
    live = counts_ref[e]

    def pack(t, carry):
        found = jnp.int32(0)
        at = [jnp.int32(0)] * slots
        for j in range(nblocks):
            hit = jnp.logical_and(dest_ref[e, j] == t, j < live)
            for s in range(slots):
                at[s] = jnp.where(jnp.logical_and(hit, found == s), j, at[s])
            found = found + hit.astype(jnp.int32)
        for s in range(slots):
            out_ref[t, s] = part_ref[at[s]]
        return carry

    lax.fori_loop(0, groups, pack, 0)
    greeted()

    def peer(d):
        return (e + d) % groups

    def exchange(t, s):
        return remote(
            out_ref.at[t], in_ref.at[s], sent.at[t], came.at[s], {"dp": t, "comp": c}
        )

    def send(d, carry):
        exchange(peer(d), e).start()
        return carry

    lax.fori_loop(1, groups, send, 0)
    in_ref[e] = out_ref[e]

    def locate(s, state):
        place, froms = state
        number = counts_ref[s]
        hits = jnp.int32(0)
        for j in range(nblocks):
            hit = jnp.logical_and(dest_ref[s, j] == e, j < number)
            hits = hits + hit.astype(jnp.int32)
        froms = list(froms)
        for q in range(slots):
            alive = q < hits
            for p in range(places):
                froms[p] = jnp.where(jnp.logical_and(alive, place == p), s * slots + q, froms[p])
            place = place + alive.astype(jnp.int32)
        return place, tuple(froms)

    _, froms = lax.fori_loop(
        0, groups, locate, (jnp.int32(0), (jnp.int32(0),) * places)
    )

    def arrived(d, carry):
        exchange(peer(d), peer(d)).wait_recv()
        return carry

    lax.fori_loop(1, groups, arrived, 0)
    for p in range(places):
        mine_ref[p] = in_ref[froms[p] // slots, froms[p] % slots]

    def block(owner, column):
        return x_ref.at[owner, :, column]

    def spread(t, s):
        return remote(
            mine_ref, block(s, c), spread_sent.at[t], spread_came.at[s], {"dp": t, "comp": c}
        )

    def spread_out(d, carry):
        spread(peer(d), e).start()
        return carry

    lax.fori_loop(1, groups, spread_out, 0)
    own = pltpu.make_async_copy(mine_ref, block(e, c), own_sem)
    own.start()

    bits = [1 << b for b in reversed(range(comps.bit_length() - 1))]

    def hop(level, index, owner, column):
        src = block(owner, column)
        return remote(
            src, src, pair_sent.at[level, index, owner], pair_came.at[level, index, owner],
            {"dp": e, "comp": c ^ bits[level]},
        )

    own.wait()
    columns = [c]
    for level in range(len(bits)):
        def forward(d, carry, level=level, columns=tuple(columns)):
            owner = peer(d)
            if level == 0:
                @pl.when(d > 0)
                def _():
                    spread(owner, owner).wait_recv()
            for index, column in enumerate(columns):
                if level > 0 and index >= len(columns) // 2:
                    hop(level - 1, index - len(columns) // 2, owner, column).wait_recv()
                hop(level, index, owner, column).start()
            return carry

        lax.fori_loop(0, groups, forward, 0)
        columns = columns + [column ^ bits[level] for column in columns]

    last = len(bits) - 1

    def finish(d, carry):
        owner = peer(d)
        for index, column in enumerate(columns[len(columns) // 2:]):
            hop(last, index, owner, column).wait_recv()
        for level in range(len(bits)):
            for index in range(1 << level):
                hop(level, index, owner, columns[index]).wait_send()

        @pl.when(d > 0)
        def _():
            exchange(owner, owner).wait_send()
            spread(owner, owner).wait_send()

        return carry

    lax.fori_loop(0, groups, finish, 0)


def merge_stage(lse_ref, total_ref, near_ref, part_ref, all_ref, near_sems, sent, came):
    comps = lax.axis_size("comp")
    devices = device_count()
    me = here()
    half = near_ref.shape[1]
    which = me % 2

    def cut(part):
        return pl.ds(pl.multiple_of(part * half, half), half)

    near = remote(
        lse_ref.at[:, cut(1 - which)], near_ref, near_sems.at[0], near_sems.at[1],
        device(me + 1 - 2 * which),
    )
    near.start()
    near.wait()
    mine = lse_ref[:, cut(which)]
    other = near_ref[...]
    peak = jnp.maximum(mine, other)
    part = peak + jnp.log(jnp.exp(mine - peak) + jnp.exp(other - peak))
    part_ref[...] = part

    def row(source):
        return all_ref.at[source % 2, pl.ds(source // 2, 1)]

    def far(target, source):
        return remote(part_ref, row(source), sent.at[target], came.at[source], device(target))

    def send(d, carry):
        far((me + d) % devices, me).start()
        return carry

    lax.fori_loop(1, devices, send, 0)
    all_ref[which, pl.ds(me // 2, 1)] = part

    def arrived(d, carry):
        source = (me + d) % devices
        far(source, source).wait_recv()
        return carry

    lax.fori_loop(1, devices, arrived, 0)
    for h in range(2):
        values = all_ref[h]
        peak = jnp.max(values, axis=0, keepdims=True)
        total_ref[:, h * half : (h + 1) * half] = peak + jnp.log(
            jnp.sum(jnp.exp(values - peak), axis=0, keepdims=True)
        )

    def left(d, carry):
        target = (me + d) % devices
        far(target, target).wait_send()
        return carry

    lax.fori_loop(1, devices, left, 0)


def merge_scratch(total):
    devices = device_count()
    return [
        pltpu.VMEM((1, total // 2), jnp.float32),
        pltpu.VMEM((1, total // 2), jnp.float32),
        pltpu.VMEM((2, devices // 2, total // 2), jnp.float32),
        pltpu.SemaphoreType.DMA((2,)),
        pltpu.SemaphoreType.DMA((devices,)),
        pltpu.SemaphoreType.DMA((devices,)),
    ]


def chunk_of(total):
    return math.gcd(total, 1024)


def eye_mask(width):
    rows = lax.broadcasted_iota(jnp.int32, (width, width), 0)
    cols = lax.broadcasted_iota(jnp.int32, (width, width), 1)
    return rows == cols


def density_stage(xt_ref, mu_ref, p_ref, w_ref, table_ref, lse_ref):
    width, total = xt_ref.shape
    members = p_ref.shape[0]
    chunk = chunk_of(total)
    diagonal = eye_mask(width)

    def member(b, carry):
        factor = p_ref[b]
        diag = jnp.sum(jnp.where(diagonal, factor, 0.0), axis=0, keepdims=True)
        logdet = jnp.sum(jnp.log(diag), axis=1, keepdims=True)
        offset = w_ref[b] + logdet - 0.5 * width * log_two_pi
        centre = mu_ref[b]
        factor_t = factor.T

        def piece(c, carry):
            cols = pl.ds(pl.multiple_of(c * chunk, chunk), chunk)
            z = xt_ref[:, cols] - centre
            y = jnp.dot(
                factor_t, z, precision=density_precision, preferred_element_type=jnp.float32
            )
            table_ref[b, :, cols] = offset - 0.5 * jnp.sum(y * y, axis=0, keepdims=True)
            return carry

        return lax.fori_loop(0, total // chunk, piece, carry)

    lax.fori_loop(0, members, member, 0)

    table = table_ref[...]
    peak = jnp.max(table, axis=0)
    lse_ref[...] = peak + jnp.log(jnp.sum(jnp.exp(table - peak[None]), axis=0))


def eliminate(m_ref, l_ref, width):
    lane = lax.broadcasted_iota(jnp.int32, (8, width), 1)

    def spread(v, j):
        return jnp.take_along_axis(v, jnp.full((8, width), j, jnp.int32), axis=1)

    def row(j):
        return pl.ds(pl.multiple_of(j * 8, 8), 8)

    def ready(value, j):
        pivot = spread(value, j)
        ahead = spread(value, jnp.minimum(j + 1, width - 1))
        scaled = jnp.where(lane == j, 1.0, value) * (1.0 / pivot)
        kept = jnp.where(lane < j, value, jnp.where(lane == j, 1.0, 0.0))
        root = lax.rsqrt(pivot)
        root = root * (1.5 - 0.5 * pivot * root * root)
        l_ref[row(j), :] = kept * root
        return scaled, ahead

    state = ready(m_ref[row(0), :], 0)
    for start in range(0, width, PANEL):

        def pivot_step(j, state, start=start):
            scaled, ahead = state
            here = lane == j
            following = jnp.where(here, 0.0, m_ref[row(j + 1), :]) - ahead * scaled
            for i in range(start + 2, width):
                old = m_ref[i * 8 : i * 8 + 8, :]
                new = jnp.where(here, 0.0, old) - spread(old, j) * scaled
                if i < start + PANEL + 1:
                    new = jnp.where(jnp.full((8, width), i, jnp.int32) > j + 1, new, old)
                m_ref[i * 8 : i * 8 + 8, :] = new
            return ready(following, j + 1)

        state = lax.fori_loop(start, min(start + PANEL, width - 1), pivot_step, state)


def update_stage(
    total_points, xt_ref, table_ref, total_ref, mu_ref,
    new_mu_ref, new_p_ref, new_w_ref, resp_ref, m_ref, l_ref,
):
    width, total = xt_ref.shape
    members = mu_ref.shape[0]
    chunk = chunk_of(total)
    log_total = total_ref[...]
    resp_ref[...] = jnp.exp(table_ref[...] - log_total[None])
    diagonal = eye_mask(width)
    identity = jnp.where(diagonal, 1.0, 0.0)

    def batch(b):
        return pl.ds(b, width, stride=8)

    for b in range(members, 8):
        m_ref[batch(b), :] = identity

    def member(b, carry):
        centre = mu_ref[b]

        def piece(c, sums):
            second, first = sums
            cols = pl.ds(pl.multiple_of(c * chunk, chunk), chunk)
            z = xt_ref[:, cols] - centre
            weighted = z * resp_ref[b, :, cols]
            second += lax.dot_general(
                weighted, z, (((1,), (1,)), ((), ())),
                precision=moment_precision, preferred_element_type=jnp.float32,
            )
            return second, first + jnp.sum(weighted, axis=1, keepdims=True)

        second, first = lax.fori_loop(
            0, total // chunk, piece,
            (jnp.zeros((width, width), jnp.float32), jnp.zeros((width, 1), jnp.float32)),
        )
        counted = jnp.sum(resp_ref[b], axis=1, keepdims=True) + 1.0
        column = jnp.broadcast_to(first, (width, width))
        covariance = (second - column * column.T / counted + identity) / counted
        m_ref[batch(b), :] = covariance
        new_mu_ref[b] = centre + first / counted
        new_w_ref[b] = jnp.log(counted / total_points)
        return carry

    lax.fori_loop(0, members, member, 0)
    eliminate(m_ref, l_ref, width)

    def emit(b, carry):
        new_p_ref[b] = l_ref[batch(b), :].T
        return carry

    lax.fori_loop(0, members, emit, 0)


def first_kernel(
    counts_ref, dest_ref, points_ref, mu_ref, p_ref, w_ref,
    xt_ref, table_ref, total_ref, x_ref, lse_ref, *scratch,
):
    greet()
    gather_stage(counts_ref, dest_ref, points_ref, x_ref, *scratch[:12])
    width, total = xt_ref.shape
    flat = x_ref.reshape(total, width)
    chunk = math.gcd(total, 512)

    def flip(c, carry):
        at = pl.ds(pl.multiple_of(c * chunk, chunk), chunk)
        xt_ref[:, at] = flat[at, :].T
        return carry

    lax.fori_loop(0, total // chunk, flip, 0)
    density_stage(xt_ref, mu_ref, p_ref, w_ref, table_ref, lse_ref)
    merge_stage(lse_ref, total_ref, *scratch[12:])


def middle_kernel(
    total_points, xt_ref, table_ref, total_ref, mu_ref,
    new_mu_ref, new_p_ref, new_w_ref, new_table_ref, new_total_ref,
    lse_ref, resp_ref, m_ref, l_ref, *scratch,
):
    greet()
    update_stage(
        total_points, xt_ref, table_ref, total_ref, mu_ref,
        new_mu_ref, new_p_ref, new_w_ref, resp_ref, m_ref, l_ref,
    )
    density_stage(xt_ref, new_mu_ref, new_p_ref, new_w_ref, new_table_ref, lse_ref)
    greeted()
    merge_stage(lse_ref, new_total_ref, *scratch)


def last_kernel(total_points, *refs):
    update_stage(total_points, *refs)


def f32(*shape):
    return jax.ShapeDtypeStruct(shape, jnp.float32)


def call(kernel, out_shape, *args, scratch=(), specs=None, params=PARAMS):
    return pl.pallas_call(
        kernel,
        out_shape=out_shape,
        in_specs=specs or [VMEM] * len(args),
        out_specs=jax.tree.map(lambda _: VMEM, out_shape),
        scratch_shapes=list(scratch),
        compiler_params=params,
    )(*args)


RB = 4


def per_device(points, block_counts, block_dest, means, factors, log_weights):
    members, width = means.shape
    groups = lax.axis_size("dp")
    comps = lax.axis_size("comp")
    nblocks = block_dest.shape[1]
    rows = points.shape[0] // nblocks
    slots = (nblocks + groups - 1) // groups
    share = rows // comps
    total = groups * RB * rows
    total_points = float(total + members * groups * comps)
    mu = means.reshape(members, width, 1)
    weights = log_weights.reshape(members, 1, 1)
    dma = pltpu.SemaphoreType.DMA
    levels = comps.bit_length() - 1
    gather_scratch = [
        pltpu.VMEM((nblocks, share, width), jnp.float32),
        pltpu.VMEM((groups, slots, share, width), jnp.float32),
        pltpu.VMEM((groups, slots, share, width), jnp.float32),
        pltpu.VMEM((RB, share, width), jnp.float32),
        dma, dma((groups,)), dma((groups,)), dma((groups,)), dma((groups,)),
        dma((levels, comps // 2, groups)), dma((levels, comps // 2, groups)), dma,
    ]
    x_scratch = pltpu.VMEM((groups, RB, comps, share, width), jnp.float32)
    lse_scratch = pltpu.VMEM((1, total), jnp.float32)
    xt, table, log_total = call(
        first_kernel, (f32(width, total), f32(members, 1, total), f32(1, total)),
        block_counts, block_dest, points.reshape(nblocks, rows, width), mu, factors, weights,
        specs=[SMEM, SMEM, ANY, VMEM, VMEM, VMEM],
        scratch=[x_scratch, lse_scratch] + gather_scratch + merge_scratch(total),
        params=talking(0),
    )
    scratch = [
        pltpu.VMEM((members, 1, total), jnp.float32),
        pltpu.VMEM((width * 8, width), jnp.float32),
        pltpu.VMEM((width * 8, width), jnp.float32),
    ]
    params = (f32(members, width, 1), f32(members, width, width), f32(members, 1, 1))
    for iteration in range(ITERS - 1):
        mu, factor, weights, table, log_total = call(
            lambda *refs: middle_kernel(total_points, *refs),
            params + (f32(members, 1, total), f32(1, total)),
            xt, table, log_total, mu,
            scratch=[lse_scratch] + scratch + merge_scratch(total),
            params=talking(1 + iteration),
        )
    mu, factor, weights = call(
        lambda *refs: last_kernel(total_points, *refs),
        params, xt, table, log_total, mu, scratch=scratch,
    )
    own = total // groups
    mine = lax.dynamic_slice_in_dim(log_total.reshape(total), lax.axis_index("dp") * own, own)
    return (mu.reshape(members, width), factor, weights.reshape(members), mine / width)


def solution(mesh):
    in_specs = (
        P("dp", None),
        P(),
        P(),
        P(("dp", "comp"), None),
        P(("dp", "comp"), None, None),
        P(("dp", "comp")),
    )
    out_specs = (P(("dp", "comp"), None), P(("dp", "comp"), None, None), P(("dp", "comp")), P("dp"))
    return jax.shard_map(
        per_device, mesh=mesh, in_specs=in_specs, out_specs=out_specs, check_vma=False
    )
```
